32 devices in a mesh: bank: 4 (over z), zero: 8 (over y, x, core).
Axes of the slice: x: 2, y: 2, z: 4, core: 2. Of those that a mesh axis runs over, the one named last changes fastest.
Arguments:
- train_gate: float32 [64, 2048, 1408], P('bank', 'zero'), may hold values from -0.1875 to 0.1875
- train_up: float32 [64, 2048, 1408], P('bank', 'zero'), may hold values from -0.1875 to 0.1875
- router_weight: float32 [2048, 64], P('zero', 'bank'), may hold values from -0.125 to 0.125
- router_gain: float32 [2048], P('zero'), may hold values from 0.25 to 1.75
Outputs:
- ready_gate: bfloat16 [64, 2048, 1408], P('bank', None, 'zero')
- ready_up: bfloat16 [64, 2048, 1408], P('bank', None, 'zero')
- scale_gate: float32 [64, 1408], P('bank', 'zero')
- scale_up: float32 [64, 1408], P('bank', 'zero')
- serve_router: bfloat16 [2048, 64], replicated
The draws below stay inside these ranges and needn't reach their ends.
All inputs are finite; a program needn't handle non-finite values. Where the reference program divides by a largest or mean magnitude, that divisor is 1e-20 or more.
Results may differ from the reference program's by a relative error of at most 0.012.
Values may be sent and summed in bfloat16 or wider, within the bound.
A program may use at most 192 MiB of HBM per device.

```python
import jax
import jax.numpy as jnp

EXPERTS = 64
D_MODEL = 2048
D_EXPERT = 1408


def spiked(result, key, source, target, blocks, factor):
    def block_of(axis_at):
        return (jnp.arange(result.shape[axis_at]) // (result.shape[axis_at] // blocks)).reshape((-1,) + (1,) * (result.ndim - 1 - axis_at))

    one_side = jax.random.permutation(key, blocks)[block_of(target)]
    other_side = (block_of(target) + blocks // 2) % blocks
    return jnp.where((block_of(source) == one_side) | (block_of(source) == other_side), factor * result, result)


def level_of(own_key, dims, pieces, low, top_value):
    def one(position, shards_of):
        steps = jax.random.uniform(jax.random.fold_in(jax.random.fold_in(own_key, 6), position), (shards_of,), jnp.float32, low / len(pieces), top_value / len(pieces))
        return jnp.repeat(jnp.exp(steps), dims[position] // shards_of).reshape((-1,) + (1,) * (len(dims) - position - 1))

    loudness = one(*pieces[0])
    for cut in pieces[1:]:
        loudness = loudness * one(*cut)
    return loudness


def gaussian(stream_key, dims, deviation, reach, pieces=(), dtype=jnp.bfloat16):
    values = jax.random.normal(stream_key, dims, jnp.float32) * deviation
    if len(pieces) > 0:
        values = level_of(stream_key, dims, pieces, -0.22, 0.18) * values
    return jnp.clip(values, min=-reach, max=reach).astype(dtype)


def noise_with(key, shape, spread, limit, cuts, heavy, kind=jnp.bfloat16):
    drawn = spread * jax.random.normal(key, shape, jnp.float32)
    if cuts:
        drawn = drawn * level_of(key, shape, cuts, -0.22, 0.18)
    return jnp.clip(spiked(drawn, jax.random.fold_in(key, 3), *heavy), -limit, limit).astype(kind)


def setup_inputs(seed: int = 0) -> dict:
    key_list = jax.random.split(jax.random.key(seed), 5)
    return {
        "train_gate": noise_with(key_list[0], (EXPERTS, D_MODEL, D_EXPERT), D_MODEL ** -0.5, 0.1875, ((0, 4), (1, 8)), (1, 2, 8, 2.0), jnp.float32),
        "train_up": noise_with(key_list[1], (EXPERTS, D_MODEL, D_EXPERT), D_MODEL ** -0.5, 0.1875, ((0, 4), (1, 8)), (1, 2, 8, 2.0), jnp.float32),
        "router_weight": gaussian(key_list[2], (D_MODEL, EXPERTS), D_MODEL ** -0.5, 0.125, ((0, 8), (1, 4)), jnp.float32),
        "router_gain": jnp.clip(1.0 + 0.15 * jax.random.normal(key_list[3], (D_MODEL,), jnp.float32), 0.25, 1.75),
    }


def reference(train_gate, train_up, router_weight, router_gain):
    scale_gate = jnp.sum(jnp.abs(train_gate), axis=1) / D_MODEL
    ready_gate = (train_gate / jnp.expand_dims(scale_gate, 1)).astype(jnp.bfloat16)
    scale_up = jnp.sum(jnp.abs(train_up), axis=1) / D_MODEL
    ready_up = (train_up / jnp.expand_dims(scale_up, 1)).astype(jnp.bfloat16)
    serve_router = (router_weight * router_gain[:, None]).astype(jnp.bfloat16)
    return ready_gate, ready_up, scale_gate, scale_up, serve_router
```

```python
import functools

import jax
import jax.numpy as jnp
from jax import lax
from jax.experimental import pallas as pl
from jax.experimental.pallas import tpu as pltpu
from jax.sharding import PartitionSpec as P

MESH = pl.DeviceIdType.MESH
LANES = 128
SLOTS = 8


def exchange(
    n, nb, gate, up, weight, gain, recv, router, inbuf, turned, send, part,
    in_sem, own_sem, send_sem, recv_sem, bank_send, bank_recv, zero_send, zero_recv,
):
    experts, rows, cols = gate.shape
    width = cols // n
    steps = 2 * experts
    slots = send.shape[0]
    me = lax.axis_index("zero")
    bank = lax.axis_index("bank")

    def fetch(source, e, slot):
        return pltpu.make_async_copy(source.at[e], inbuf.at[slot], in_sem.at[slot])

    fetch(gate, 0, 0).start()
    fetch(up, 0, 1).start()

    barrier = pltpu.get_barrier_semaphore()
    for k in range(1, n):
        pl.semaphore_signal(barrier, inc=1, device_id={"zero": lax.rem(me + k, n)}, device_id_type=MESH)
    for k in range(1, nb):
        pl.semaphore_signal(barrier, inc=1, device_id={"bank": lax.rem(bank + k, nb)}, device_id_type=MESH)
    part[...] = (weight[...] * gain[...]).astype(part.dtype)

    def own_copy(t, slot):
        return pltpu.make_async_copy(send.at[slot, me], recv.at[me, t], own_sem.at[slot])

    def peer_copy(t, slot, k):
        peer = lax.rem(me + k, n)
        return pltpu.make_async_remote_copy(
            src_ref=send.at[slot, peer],
            dst_ref=recv.at[me, t],
            send_sem=send_sem.at[slot, k],
            recv_sem=recv_sem.at[k],
            device_id={"zero": peer},
            device_id_type=MESH,
        )

    def turn(half, slot):
        for j in range(0, cols, LANES):
            turned[j : j + LANES, :] = inbuf[half, :, j : j + LANES].T
        for d in range(n):
            send[slot, d] = turned[d * width : (d + 1) * width, :].astype(send.dtype)

    def drain(t, slot):
        own_copy(t, slot).wait()
        for k in range(1, n):
            peer_copy(t, slot, k).wait_send()

    def launch(t, slot):
        for k in range(1, n):
            peer_copy(t, slot, k).start()
        own_copy(t, slot).start()

    def column(z):
        return pl.ds(pl.multiple_of(z * rows, rows), rows)

    def bank_copy(k):
        return pltpu.make_async_remote_copy(
            src_ref=part,
            dst_ref=router.at[bank, :, column(me)],
            send_sem=bank_send.at[k],
            recv_sem=bank_recv.at[k],
            device_id={"bank": lax.rem(bank + k, nb)},
            device_id_type=MESH,
        )

    def zero_copy(k):
        return pltpu.make_async_remote_copy(
            src_ref=router.at[:, :, column(me)],
            dst_ref=router.at[:, :, column(me)],
            send_sem=zero_send.at[k],
            recv_sem=zero_recv.at[k],
            device_id={"zero": lax.rem(me + k, n)},
            device_id_type=MESH,
        )

    fetch(gate, 0, 0).wait()
    turn(0, 0)
    pl.semaphore_wait(barrier, n - 1 + nb - 1)

    router[bank, :, column(me)] = part[...]
    for k in range(1, nb):
        bank_copy(k).start()

    @pl.loop(0, experts)
    def _(e):
        for half, source in enumerate((gate, up)):
            t = 2 * e + half
            slot = lax.rem(t, slots)

            def ready():
                fetch(source, e, half).wait()

                @pl.when(t >= slots)
                def _():
                    drain(t - slots, slot)

                turn(half, slot)

            if half == 0:
                pl.when(e > 0)(ready)
            else:
                ready()
            launch(t, slot)

            @pl.when(e + 1 < experts)
            def _():
                fetch(source, e + 1, half).start()

        @pl.when(e == min(1, experts - 1))
        def _():
            for k in range(1, nb):
                bank_copy(k).wait()
            for k in range(1, n):
                zero_copy(k).start()

    for k in range(1, n):
        zero_copy(k).wait()

    @pl.loop(max(steps - slots, 0), steps)
    def _(t):
        drain(t, lax.rem(t, slots))

    for k in range(1, n):
        source = lax.rem(me - k + n, n)
        pltpu.make_async_remote_copy(
            src_ref=recv.at[source],
            dst_ref=recv.at[source],
            send_sem=send_sem.at[0, 0],
            recv_sem=recv_sem.at[k],
            device_id={"zero": source},
            device_id_type=MESH,
        ).wait_recv()


def finish(n, d_model, got, ready_gate, ready_up, scale_gate, scale_up, wide):
    e = pl.program_id(0)
    width, rows = got.shape[2], got.shape[3]
    for half, (ready, scale) in enumerate(((ready_gate, scale_gate), (ready_up, scale_up))):
        total = jnp.zeros((width, LANES), jnp.float32)
        for s in range(n):
            for j in range(0, rows, LANES):
                total += jnp.abs(got[s, half, :, j : j + LANES].astype(jnp.float32))
        mean = jnp.sum(total, axis=1, keepdims=True) / d_model
        wide[0:width, :] = jnp.broadcast_to(mean, (width, LANES))
        for j in range(0, width, LANES):
            stop = min(j + LANES, width)
            line = wide[j : j + LANES, :].T[0:1, 0 : stop - j]
            mine = lax.broadcasted_iota(jnp.int32, (scale.shape[0], stop - j), 0) == e
            scale[:, j:stop] = jnp.where(mine, line, scale[:, j:stop])
        inverse = jnp.broadcast_to(1.0 / mean, (width, LANES))
        for s in range(n):
            for j in range(0, rows, LANES):
                value = got[s, half, :, j : j + LANES].astype(jnp.float32) * inverse
                ready[0, :, s * rows + j : s * rows + j + LANES] = value.astype(ready.dtype)


def solution(mesh):
    n, nb = mesh.shape["zero"], mesh.shape["bank"]

    def local(train_gate, train_up, router_weight, router_gain):
        experts, rows, cols = train_gate.shape
        width = cols // n
        d_model = rows * n
        mine = router_weight.shape[1]
        slots = min(SLOTS, 2 * experts)
        anywhere = pl.BlockSpec(memory_space=pl.ANY)
        inside = pl.BlockSpec(memory_space=pltpu.VMEM)
        recv, router = pl.pallas_call(
            functools.partial(exchange, n, nb),
            out_shape=(
                jax.ShapeDtypeStruct((n, 2 * experts, width, rows), jnp.bfloat16),
                jax.ShapeDtypeStruct((nb, mine, d_model), jnp.bfloat16),
            ),
            in_specs=[anywhere, anywhere, inside, inside],
            out_specs=(anywhere, inside),
            scratch_shapes=[
                pltpu.VMEM((2, rows, cols), jnp.float32),
                pltpu.VMEM((cols, rows), jnp.float32),
                pltpu.VMEM((slots, n, width, rows), jnp.bfloat16),
                pltpu.VMEM((mine, rows), jnp.bfloat16),
                pltpu.SemaphoreType.DMA((2,)),
                pltpu.SemaphoreType.DMA((slots,)),
                pltpu.SemaphoreType.DMA((slots, n)),
                pltpu.SemaphoreType.DMA((n,)),
                pltpu.SemaphoreType.DMA((nb,)),
                pltpu.SemaphoreType.DMA((nb,)),
                pltpu.SemaphoreType.DMA((n,)),
                pltpu.SemaphoreType.DMA((n,)),
            ],
            compiler_params=pltpu.CompilerParams(collective_id=0, has_side_effects=True),
        )(train_gate, train_up, router_weight.T, router_gain[None, :])

        padded = -(-width // LANES) * LANES
        ready = jax.ShapeDtypeStruct((experts, width, d_model), jnp.bfloat16)
        scale = jax.ShapeDtypeStruct((experts, width), jnp.float32)
        ready_spec = pl.BlockSpec((1, width, d_model), lambda e: (e, 0, 0))
        scale_spec = pl.BlockSpec((experts, width), lambda e: (0, 0))
        ready_gate, ready_up, scale_gate, scale_up = pl.pallas_call(
            functools.partial(finish, n, d_model),
            grid=(experts,),
            out_shape=(ready, ready, scale, scale),
            in_specs=[pl.BlockSpec((n, 2, width, rows), lambda e: (0, e, 0, 0))],
            out_specs=(ready_spec, ready_spec, scale_spec, scale_spec),
            scratch_shapes=[pltpu.VMEM((padded, LANES), jnp.float32)],
        )(recv)
        return (
            jnp.swapaxes(ready_gate, 1, 2),
            jnp.swapaxes(ready_up, 1, 2),
            scale_gate,
            scale_up,
            router.reshape(nb * mine, d_model).T,
        )

    in_specs = (P("bank", "zero", None), P("bank", "zero", None), P("zero", "bank"), P("zero"))
    out_specs = (
        P("bank", None, "zero"),
        P("bank", None, "zero"),
        P("bank", "zero"),
        P("bank", "zero"),
        P(),
    )
    return jax.shard_map(local, mesh=mesh, in_specs=in_specs, out_specs=out_specs, check_vma=False)
```

```python
import functools

import jax
import jax.numpy as jnp
from jax import lax
from jax.experimental import pallas as pl
from jax.experimental.pallas import tpu as pltpu
from jax.sharding import PartitionSpec as P

MESH = pl.DeviceIdType.MESH
LANES = 128
SLOTS = 8
LAG = 5
KERNEL_VMEM = 28 * 2**20
FINISH_VMEM = 2 * 2**20


def exchange(
    n, nb, gate, up, weight, gain, recv, router, scale_gate, scale_up, inbuf, turned, send, part, wide,
    in_sem, send_sem, recv_sem, bank_send, bank_recv, zero_send, zero_recv,
):
    experts, rows, cols = gate.shape
    width = cols // n
    steps = 2 * experts
    slots = send.shape[0]
    lag = min(LAG, experts)
    me = lax.axis_index("zero")
    bank = lax.axis_index("bank")

    def fetch(source, e, slot):
        return pltpu.make_async_copy(source.at[e], inbuf.at[slot], in_sem.at[slot])

    fetch(gate, 0, 0).start()
    fetch(up, 0, 1).start()

    barrier = pltpu.get_barrier_semaphore()
    for k in range(1, n):
        pl.semaphore_signal(barrier, inc=1, device_id={"zero": lax.rem(me + k, n)}, device_id_type=MESH)
    for k in range(1, nb):
        pl.semaphore_signal(barrier, inc=1, device_id={"bank": lax.rem(bank + k, nb)}, device_id_type=MESH)
    scale_gate[...] = jnp.zeros_like(scale_gate)
    scale_up[...] = jnp.zeros_like(scale_up)
    part[...] = (weight[...] * gain[...]).astype(part.dtype)

    def peer_copy(half, e, slot, k):
        peer = lax.rem(me + k, n)
        return pltpu.make_async_remote_copy(
            src_ref=send.at[slot, peer],
            dst_ref=recv.at[me, half, e],
            send_sem=send_sem.at[slot, k],
            recv_sem=recv_sem.at[e, k],
            device_id={"zero": peer},
            device_id_type=MESH,
        )

    def turn(half, slot):
        for j in range(0, cols, LANES):
            turned[j : j + LANES, :] = inbuf[half, :, j : j + LANES].T
        for d in range(n):
            send[slot, d] = turned[d * width : (d + 1) * width, :].astype(send.dtype)

    def drain(slot):
        for k in range(1, n):
            peer_copy(0, 0, slot, k).wait_send()

    def launch(half, e, slot):
        for k in range(1, n):
            peer_copy(half, e, slot, k).start()
        recv[me, half, e] = send[slot, me]

    def settle(e):
        for k in range(1, n):
            source = lax.rem(me - k + n, n)
            pltpu.make_async_remote_copy(
                src_ref=recv.at[source, :, e],
                dst_ref=recv.at[source, :, e],
                send_sem=send_sem.at[0, 0],
                recv_sem=recv_sem.at[e, k],
                device_id={"zero": source},
                device_id_type=MESH,
            ).wait_recv()
        for half, scale in enumerate((scale_gate, scale_up)):
            total = jnp.zeros((width, LANES), jnp.float32)
            for s in range(n):
                for j in range(0, rows, LANES):
                    total += jnp.abs(recv[s, half, e, :, j : j + LANES].astype(jnp.float32))
            mean = jnp.sum(total, axis=1, keepdims=True) / (rows * n)
            wide[0:width, :] = jnp.broadcast_to(mean, (width, LANES))
            for j in range(0, width, LANES):
                stop = min(j + LANES, width)
                line = wide[j : j + LANES, :].T[0:1, 0 : stop - j]
                here = lax.broadcasted_iota(jnp.int32, (experts, stop - j), 0) == e
                scale[:, j:stop] = jnp.where(here, line, scale[:, j:stop])
            inverse = jnp.broadcast_to(1.0 / mean, (width, LANES))
            for s in range(n):
                for j in range(0, rows, LANES):
                    value = recv[s, half, e, :, j : j + LANES].astype(jnp.float32) * inverse
                    recv[s, half, e, :, j : j + LANES] = value.astype(recv.dtype)

    def column(z):
        return pl.ds(pl.multiple_of(z * rows, rows), rows)

    def bank_copy(k):
        return pltpu.make_async_remote_copy(
            src_ref=part,
            dst_ref=router.at[bank, :, column(me)],
            send_sem=bank_send.at[k],
            recv_sem=bank_recv.at[k],
            device_id={"bank": lax.rem(bank + k, nb)},
            device_id_type=MESH,
        )

    def zero_copy(k):
        return pltpu.make_async_remote_copy(
            src_ref=router.at[:, :, column(me)],
            dst_ref=router.at[:, :, column(me)],
            send_sem=zero_send.at[k],
            recv_sem=zero_recv.at[k],
            device_id={"zero": lax.rem(me + k, n)},
            device_id_type=MESH,
        )

    fetch(gate, 0, 0).wait()
    turn(0, 0)
    pl.semaphore_wait(barrier, n - 1 + nb - 1)

    router[bank, :, column(me)] = part[...]
    for k in range(1, nb):
        bank_copy(k).start()

    @pl.loop(0, experts)
    def _(e):
        for half, source in enumerate((gate, up)):
            t = 2 * e + half
            slot = lax.rem(t, slots)

            def ready():
                fetch(source, e, half).wait()

                @pl.when(t >= slots)
                def _():
                    drain(slot)

                turn(half, slot)

            if half == 0:
                pl.when(e > 0)(ready)
            else:
                ready()
            launch(half, e, slot)

            @pl.when(e + 1 < experts)
            def _():
                fetch(source, e + 1, half).start()

        @pl.when(e == min(1, experts - 1))
        def _():
            for k in range(1, nb):
                bank_copy(k).wait()
            for k in range(1, n):
                zero_copy(k).start()

        @pl.when(e >= lag)
        def _():
            settle(e - lag)

    @pl.loop(experts - lag, experts)
    def _(e):
        settle(e)

    for k in range(1, n):
        zero_copy(k).wait()

    @pl.loop(max(steps - slots, 0), steps)
    def _(t):
        drain(lax.rem(t, slots))


def finish(
    recv, router, scale_gate, scale_up,
    ready_gate, ready_up, router_out, scale_gate_out, scale_up_out, sem, router_sem,
):
    n, rows = recv.shape[0], recv.shape[4]
    copies = [
        pltpu.make_async_copy(recv.at[s, half], ready.at[:, :, s * rows : (s + 1) * rows], sem.at[s, half])
        for s in range(n)
        for half, ready in enumerate((ready_gate, ready_up))
    ]
    copies.append(pltpu.make_async_copy(router, router_out, router_sem))
    for copy in copies:
        copy.start()
    scale_gate_out[...] = scale_gate[...]
    scale_up_out[...] = scale_up[...]
    for copy in copies:
        copy.wait()


def solution(mesh):
    n, nb = mesh.shape["zero"], mesh.shape["bank"]

    def local(train_gate, train_up, router_weight, router_gain):
        experts, rows, cols = train_gate.shape
        width = cols // n
        d_model = rows * n
        mine = router_weight.shape[1]
        slots = min(SLOTS, 2 * experts)
        anywhere = pl.BlockSpec(memory_space=pl.ANY)
        inside = pl.BlockSpec(memory_space=pltpu.VMEM)
        padded = -(-width // LANES) * LANES
        scale = jax.ShapeDtypeStruct((experts, width), jnp.float32)
        joined = jax.ShapeDtypeStruct((nb, mine, d_model), jnp.bfloat16)
        recv, router, scale_gate, scale_up = pl.pallas_call(
            functools.partial(exchange, n, nb),
            out_shape=(
                jax.ShapeDtypeStruct((n, 2, experts, width, rows), jnp.bfloat16),
                joined,
                scale,
                scale,
            ),
            in_specs=[anywhere, anywhere, inside, inside],
            out_specs=(inside,) * 4,
            scratch_shapes=[
                pltpu.VMEM((2, rows, cols), jnp.float32),
                pltpu.VMEM((cols, rows), jnp.float32),
                pltpu.VMEM((slots, n, width, rows), jnp.bfloat16),
                pltpu.VMEM((mine, rows), jnp.bfloat16),
                pltpu.VMEM((padded, LANES), jnp.float32),
                pltpu.SemaphoreType.DMA((2,)),
                pltpu.SemaphoreType.DMA((slots, n)),
                pltpu.SemaphoreType.DMA((experts, n)),
                pltpu.SemaphoreType.DMA((nb,)),
                pltpu.SemaphoreType.DMA((nb,)),
                pltpu.SemaphoreType.DMA((n,)),
                pltpu.SemaphoreType.DMA((n,)),
            ],
            compiler_params=pltpu.CompilerParams(
                collective_id=0, has_side_effects=True, vmem_limit_bytes=KERNEL_VMEM
            ),
        )(train_gate, train_up, router_weight.T, router_gain[None, :])

        ready = jax.ShapeDtypeStruct((experts, width, d_model), jnp.bfloat16)
        ready_gate, ready_up, router, scale_gate, scale_up = pl.pallas_call(
            finish,
            out_shape=(ready, ready, joined, scale, scale),
            in_specs=[inside] * 4,
            out_specs=(anywhere, anywhere, anywhere, inside, inside),
            scratch_shapes=[pltpu.SemaphoreType.DMA((n, 2)), pltpu.SemaphoreType.DMA],
            compiler_params=pltpu.CompilerParams(vmem_limit_bytes=FINISH_VMEM),
        )(recv, router, scale_gate, scale_up)
        return (
            jnp.swapaxes(ready_gate, 1, 2),
            jnp.swapaxes(ready_up, 1, 2),
            scale_gate,
            scale_up,
            router.reshape(nb * mine, d_model).T,
        )

    in_specs = (P("bank", "zero", None), P("bank", "zero", None), P("zero", "bank"), P("zero"))
    out_specs = (
        P("bank", None, "zero"),
        P("bank", None, "zero"),
        P("bank", "zero"),
        P("bank", "zero"),
        P(),
    )
    return jax.shard_map(local, mesh=mesh, in_specs=in_specs, out_specs=out_specs, check_vma=False)
```
